768 devices in a mesh: dp: 12 (over z), rep: 8 (over y), grp: 8 (over x, core).
Axes of the slice: x: 4, y: 8, z: 12, core: 2. Of those that a mesh axis runs over, the one named last changes fastest.
Arguments:
- grad_parts: float32 [64, 24, 192, 2048], P(('rep', 'grp'), None, 'dp'), may hold values from -16 to 16
- momentum: float32 [24, 192, 2048], P(None, 'dp', ('rep', 'grp')), may hold values from -24 to 24
- layer_live: int32 [24], replicated, may hold values from 0 to 1, as said below
Outputs:
- new_momentum: float32 [24, 192, 2048], P(None, 'dp', ('rep', 'grp'))
- orth_update: bfloat16 [24, 192, 2048], P(None, 'dp', ('rep', 'grp'))
The draws below stay inside these ranges and needn't reach their ends.
Inputs may be any that keep to these rules, and one draw needn't show every extreme that they name: `layer_live`: at least one matrix is live in every draw.
All inputs are finite; a program needn't handle non-finite values.
Results may differ from the reference program's by a relative error of at most 0.028.
Values may be sent and summed in bfloat16 or wider, within the bound.
No kernel may reach another device: no remote copies, remote signals or barrier semaphores. Data moves between devices by JAX's collectives and lax.ppermute only.
A program may use at most 64 MiB of HBM per device.

```python
import math
import jax
import jax.numpy as jnp
from jax import lax

ROWS = 192
C = 2048
ITERS = 5
MATS = 24
REPLICAS = 64


def draw_layer_live(key, part):
    first_key, second_key = jax.random.split(jax.random.fold_in(key, 17))
    coin_flips = jax.random.randint(first_key, (MATS,), 0, 2, dtype=jnp.int32)
    chosen = jax.random.randint(second_key, (), 0, MATS, dtype=jnp.int32)
    forced = (jnp.arange(MATS, dtype=jnp.int32) == chosen).astype(jnp.int32)
    return jnp.maximum(coin_flips, forced)


def spiked(array, own_key, source, target, shards_of, factor):
    owner, partner = [(jnp.arange(array.shape[axis_at]) // (array.shape[axis_at] // shards_of)).reshape([-1 if axis == axis_at else 1 for axis in range(array.ndim)]) for axis_at in (source, target)]
    chosen = jax.random.permutation(own_key, shards_of)[partner]
    strong = (owner == chosen) | (owner == (partner + shards_of // 2) % shards_of)
    return jnp.where(strong, factor * array, array)


def block_levels(own_key, shape, pieces, least, largest):
    gain = 1.0
    for axis_at, shards_of in pieces:
        draws = jax.random.uniform(jax.random.fold_in(jax.random.fold_in(own_key, 6), axis_at), (shards_of,), jnp.float32, least / len(pieces), largest / len(pieces))
        gain = gain * jnp.repeat(jnp.exp(draws), shape[axis_at] // shards_of).reshape((-1,) + (1,) * (len(shape) - 1 - axis_at))
    return gain


def bell_draw(stream_key, shape, spread, most, shards=(), held_as=jnp.bfloat16):
    drawn = spread * jax.random.normal(stream_key, shape, jnp.float32)
    if shards:
        drawn = drawn * block_levels(stream_key, shape, shards, -0.22, 0.18)
    return jnp.clip(drawn, -most, most).astype(held_as)


def heavy_noise(key, shape, deviation, limit, cuts, heavy, kind=jnp.bfloat16):
    result = deviation * jax.random.normal(key, shape, jnp.float32)
    if cuts:
        result = result * block_levels(key, shape, cuts, -0.22, 0.18)
    return jnp.clip(spiked(result, jax.random.fold_in(key, 3), *heavy), -limit, limit).astype(kind)


def setup_inputs(seed: int = 0) -> dict:
    seeds = jax.random.split(jax.random.key(seed), 4)
    grad_parts = heavy_noise(seeds[0], (REPLICAS, MATS, ROWS, C), 1.0, 16.0, ((0, 64), (2, 12)), (0, 3, 64, 4.0), jnp.float32)
    momentum = bell_draw(seeds[1], (MATS, ROWS, C), 4.0, 24.0, ((1, 12), (2, 64)), jnp.float32)
    layer_live = draw_layer_live(jax.random.fold_in(seeds[3], 71), 0)
    return dict(grad_parts=grad_parts, momentum=momentum, layer_live=layer_live)


decay_rate = 0.95
first_coef = 3.4445
second_coef = -4.775
third_coef = 2.0315
norm_eps = 1e-07

def newton_schulz(source):
    source_f32 = source.astype(jnp.float32)
    frob_norm = jnp.sqrt(jnp.sum(source_f32 * source_f32))
    current = (source_f32 / (frob_norm + norm_eps)).astype(jnp.bfloat16)
    next_iterate = source_f32
    for iteration in range(ITERS):
        gram_matrix = lax.dot_general(current, current, (((1,), (1,)), ((), ())), preferred_element_type=jnp.float32).astype(jnp.bfloat16)
        squared = jnp.dot(gram_matrix, gram_matrix, preferred_element_type=jnp.float32)
        polynomial = (second_coef * gram_matrix.astype(jnp.float32) + third_coef * squared).astype(jnp.bfloat16)
        next_iterate = first_coef * current.astype(jnp.float32) + jnp.dot(polynomial, current, preferred_element_type=jnp.float32)
        if iteration + 1 < ITERS:
            current = next_iterate.astype(jnp.bfloat16)
    return (next_iterate * math.sqrt(source.shape[1])).astype(jnp.bfloat16)

def reference(grad_parts, momentum, layer_live):
    grad_sum = lax.optimization_barrier(jnp.sum(grad_parts, axis=0))
    active = (layer_live > 0)[:, None, None]
    new_momentum = jnp.where(active, decay_rate * momentum + grad_sum, momentum)
    sources = new_momentum.astype(jnp.bfloat16)
    updates = lax.map(newton_schulz, sources)
    orth_update = jnp.where(active, updates, jnp.zeros_like(updates))
    return (new_momentum, orth_update)
```

```python
import math

import jax
import jax.numpy as jnp
from jax import lax
from jax.experimental import pallas as pl
from jax.experimental.pallas import tpu as pltpu
from jax.sharding import Mesh
from jax.sharding import PartitionSpec as P

ITERS = 5
COLS = ("rep", "x1", "x0", "c")
CHIPS = ("rep", "x1", "x0")
OWNERS = ("rep", "x1")
SLOTS = 16
STEP = 4

decay_rate = 0.95
first_coef = 3.4445
second_coef = -4.775
third_coef = 2.0315
norm_eps = 1e-07

bf16 = jnp.bfloat16
f32 = jnp.float32
i32 = jnp.int32


def whole(space=pltpu.VMEM):
    return pl.BlockSpec(memory_space=space)


def pack_body(holder, *refs):
    grads, mom, out = refs[:STEP], refs[STEP], refs[STEP + 1]
    step = pl.program_id(0)
    rep, x1 = lax.axis_index("rep"), lax.axis_index("x1")
    x0, c = lax.axis_index("x0"), lax.axis_index("c")
    group = lax.broadcasted_iota(i32, (16, 128), 1) // 32
    spot = (rep % 2) * 2 + x1
    start = pl.multiple_of((rep // 2) * 128, 128)
    for k in range(STEP):
        for yy in range(4):
            tiles = [grads[k][0, 0, :, (yy * 4 + t) * 128 : (yy * 4 + t + 1) * 128] for t in range(4)]
            for q in range(4):
                dealt = None
                for t in range(4):
                    turn = ((t - q) * 32) % 128
                    moved = pltpu.roll(tiles[t], turn, 1) if turn else tiles[t]
                    dealt = moved if dealt is None else jnp.where(group == t, moved, dealt)
                out[q % 2, 2 * k + q // 2, :, yy * 128 : (yy + 1) * 128] = dealt.astype(bf16)
        own = mom[holder[step * STEP + k]] * decay_rate
        own = jnp.concatenate([own] * 4, axis=1)
        own = jnp.where(group == spot, own, 0.0)
        at = (c, 2 * k + x0, slice(None), pl.ds(start, 128))
        out[at] = (out[at].astype(f32) + own).astype(bf16)


def pack(grad_parts, momentum, holder):
    _, mats, rows, cols = grad_parts.shape
    picks = [
        pl.BlockSpec((1, 1, rows, cols), lambda i, h, k=k: (0, h[i * STEP + k], 0, 0)) for k in range(STEP)
    ]
    return pl.pallas_call(
        pack_body,
        grid_spec=pltpu.PrefetchScalarGridSpec(
            num_scalar_prefetch=1,
            grid=(SLOTS // STEP,),
            in_specs=picks + [pl.BlockSpec(momentum.shape, lambda i, h: (0, 0, 0))],
            out_specs=pl.BlockSpec((2, 2 * STEP, rows, cols // 4), lambda i, h: (0, i, 0, 0)),
        ),
        out_shape=jax.ShapeDtypeStruct((2, 2 * SLOTS, rows, cols // 4), bf16),
        name="pack",
    )(holder, *[grad_parts] * STEP, momentum)


def total_body(parts, out):
    total = jnp.sum(parts[...].astype(f32), axis=0).astype(bf16)
    for z in range(out.shape[0]):
        out[z] = total


def total(parts, copies):
    return pl.pallas_call(
        total_body,
        in_specs=[whole()],
        out_specs=whole(),
        out_shape=jax.ShapeDtypeStruct((copies,) + parts.shape[1:], bf16),
        name="total",
    )(parts)


def gram_body(source, out):
    s = source[...].reshape(out.shape[0], -1)
    out[...] = lax.dot_general(s, s, (((1,), (1,)), ((), ())), preferred_element_type=f32)


def gram(source):
    rows = source.shape[0] * source.shape[1]
    return pl.pallas_call(
        gram_body,
        in_specs=[whole()],
        out_specs=whole(),
        out_shape=jax.ShapeDtypeStruct((rows, rows), f32),
        name="gram",
    )(source)


def halves(a):
    high = a.astype(bf16)
    return high, (a - high.astype(f32)).astype(bf16)


def dot(a, b):
    return jnp.dot(a, b, preferred_element_type=f32)


def dot3(a, b):
    return dot(a[0], b[0]) + (dot(a[0], b[1]) + dot(a[1], b[0]))


def schulz_body(gram_a, gram_b, source, out):
    g = gram_a[...] + gram_b[...]
    rows = g.shape[0]
    own_rows = source.shape[1]
    z = lax.axis_index("dp")
    row = lax.broadcasted_iota(i32, g.shape, 0)
    col = lax.broadcasted_iota(i32, g.shape, 1)
    eye = row == col
    square = jnp.sum(jnp.sum(jnp.where(eye, g, 0.0), axis=1, keepdims=True), axis=0, keepdims=True)
    scale = 1.0 / (jnp.sqrt(square) + norm_eps)
    g = g * scale * scale
    pick = (
        lax.broadcasted_iota(i32, (own_rows, rows), 1)
        == lax.broadcasted_iota(i32, (own_rows, rows), 0) + z * own_rows
    )
    lead = pick.astype(bf16)
    lead = (lead, jnp.zeros_like(lead))
    for iteration in range(ITERS):
        gh = halves(g)
        w = second_coef * g + third_coef * dot3(gh, gh)
        w = w + jnp.where(eye, first_coef, 0.0)
        wh = halves(w)
        led = dot3(lead, wh)
        if iteration + 1 < ITERS:
            g = dot3(halves(dot3(wh, gh)), wh)
            lead = halves(led)
    lead = halves(led * (scale * math.sqrt(2048.0)))
    s = source[...].reshape(rows, -1)
    result = dot(lead[0], s) + dot(lead[1], s)
    own = source[z].astype(f32)
    lane = lax.broadcasted_iota(i32, (own_rows, 128), 1)
    for j in range(out.shape[0]):
        yy, t = j // 4, j % 4
        up = result[:, yy * 128 : (yy + 1) * 128]
        low = own[:, yy * 128 : (yy + 1) * 128]
        up = pltpu.roll(up, 128 - 32 * t, 1) if t else up
        low = pltpu.roll(low, (160 - 32 * t) % 128, 1) if t != 1 else low
        out[j] = jnp.where(lane < 32, up, low).astype(bf16)


def schulz(gram_a, gram_b, source):
    return pl.pallas_call(
        schulz_body,
        in_specs=[whole(), whole(), whole()],
        out_specs=whole(),
        out_shape=jax.ShapeDtypeStruct((SLOTS, source.shape[1], 128), bf16),
        name="schulz",
    )(gram_a, gram_b, source)


def place_body(slot, came, mom_in, orth_in, mom, orth):
    for m in range(mom.shape[0]):
        s = slot[m]
        here = (s >= 0) & (s < SLOTS)
        got = came[jnp.clip(s, 0, SLOTS - 1)].astype(f32)
        mom[m] = jnp.where(here, pltpu.roll(got, 96, 1)[:, :32], mom_in[m])
        orth[m] = jnp.where(here, got[:, :32], orth_in[m].astype(f32)).astype(bf16)


def place(slot, came, mom_in, orth_in):
    return pl.pallas_call(
        place_body,
        in_specs=[whole(pltpu.SMEM), whole(), whole(), whole()],
        out_specs=[whole(), whole()],
        out_shape=[jax.ShapeDtypeStruct(mom_in.shape, f32), jax.ShapeDtypeStruct(mom_in.shape, bf16)],
        name="place",
    )(slot, came, mom_in, orth_in)


def swapped(x, axis):
    return lax.ppermute(x, axis, [(0, 1), (1, 0)])


def one_pass(grad_parts, momentum, holder, slot, mom_in, orth_in):
    packed = pack(grad_parts, momentum, holder)
    both = lax.all_to_all(packed, "c", 0, 0, tiled=True)
    chip_sum = (both[0].astype(f32) + both[1].astype(f32)).astype(bf16)
    parts = lax.all_to_all(chip_sum, CHIPS, 0, 0, tiled=True)
    copies = total(parts, lax.axis_size("dp"))
    source = lax.all_to_all(copies, "dp", 0, 0, tiled=True)
    partial = gram(source)
    partial = partial + swapped(partial, "c")
    update = schulz(partial, swapped(partial, "x0"), source)
    came = lax.all_to_all(update, OWNERS, 0, 0, tiled=True)
    return place(slot, came, mom_in, orth_in)


def per_device(grad_parts, momentum, layer_live):
    mats = layer_live.shape[0]
    ids = jnp.arange(mats, dtype=i32)
    live = layer_live > 0
    rank = jnp.sum(jnp.where(live[None, :] & (ids[None, :] < ids[:, None]), 1, 0), axis=1)
    slot = jnp.where(live, rank, -1)
    places = jnp.arange(2 * SLOTS, dtype=i32)
    holder = jnp.sum(jnp.where(slot[None, :] == places[:, None], ids[None, :], 0), axis=1)
    orth = jnp.zeros(momentum.shape, bf16)
    mom, orth = one_pass(grad_parts, momentum, holder[:SLOTS], slot, momentum, orth)

    def again(mom, orth):
        return tuple(one_pass(grad_parts, momentum, holder[SLOTS:], slot - SLOTS, mom, orth))

    return lax.cond(jnp.sum(live.astype(i32)) > SLOTS, again, lambda mom, orth: (mom, orth), mom, orth)


def solution(mesh):
    torus = Mesh(
        mesh.devices.reshape(mesh.shape["dp"], mesh.shape["rep"], 2, 2, 2),
        ("dp", "rep", "x1", "x0", "c"),
    )
    return jax.shard_map(
        per_device,
        mesh=torus,
        in_specs=(P(COLS, None, "dp", None), P(None, "dp", COLS), P()),
        out_specs=(P(None, "dp", COLS), P(None, "dp", COLS)),
        check_vma=False,
    )
```

```python
import functools
import math

import jax
import jax.numpy as jnp
from jax import lax
from jax.experimental import pallas as pl
from jax.experimental.pallas import tpu as pltpu
from jax.sharding import Mesh
from jax.sharding import PartitionSpec as P

ITERS = 5
COLS = ("rep", "x1", "x0", "c")
CHIPS = ("rep", "x1", "x0")
OWNERS = ("rep", "x1")

decay_rate = 0.95
first_coef = 3.4445
second_coef = -4.775
third_coef = 2.0315
norm_eps = 1e-07

bf16 = jnp.bfloat16
f32 = jnp.float32
i32 = jnp.int32


def whole(space=pltpu.VMEM):
    return pl.BlockSpec(memory_space=space)


def room(mib):
    return pltpu.CompilerParams(vmem_limit_bytes=mib << 20)


def halves(a):
    high = a.astype(bf16)
    return high, (a - high.astype(f32)).astype(bf16)


def dot(a, b):
    return jnp.dot(a, b, preferred_element_type=f32)


def dot3(a, b):
    return dot(a[0], b[0]) + (dot(a[0], b[1]) + dot(a[1], b[0]))


def pack_body(live, grads, mom, mine, theirs, mine_wide, theirs_wide, count, rows, own_mom, holder, row_sems, mom_sem):
    slots, height, width = rows.shape
    mats = live.shape[0]
    fetch_mom = pltpu.make_async_copy(mom, own_mom, mom_sem)
    fetch_mom.start()
    for s in range(slots):
        holder[s] = 0
    found = 0
    for m in range(mats):
        holder[found] = m
        found = found + jnp.where(live[m] > 0, 1, 0)
    count[0] = found
    used = jnp.where(found > 16, slots, 16)

    def fetch(s):
        return pltpu.make_async_copy(grads.at[0, holder[s]], rows.at[s], row_sems.at[s])

    def begin(s, _):
        fetch(s).start()
        return 0

    lax.fori_loop(0, used, begin, 0)
    rep, x1 = lax.axis_index("rep"), lax.axis_index("x1")
    x0, c = lax.axis_index("x0"), lax.axis_index("c")
    group = lax.broadcasted_iota(i32, (height, 128), 1) // 32
    start = pl.multiple_of((rep * 2 + x1) * 128, 128)
    fetch_mom.wait()

    def spread(slots, block, near, far):
        blocks = width // block
        old = lax.broadcasted_iota(i32, (block, block), 0)
        new = lax.broadcasted_iota(i32, (block, block), 1)
        far_half = ((old // 32 % 2) ^ c) * (block // 2)
        if block == 512:
            target = far_half + (old // 64 % 2) * 128 + old // 128 * 32 + old % 32
        else:
            target = far_half + old // 128 * 64 + (old // 64 % 2) * 32 + old % 32
        deal = jnp.where(target == new, 1.0, 0.0).astype(bf16)

        def four(g, _):
            lead = []
            for k in range(4):
                s = g * 4 + k
                fetch(s).wait()
                own = own_mom[holder[s]] * decay_rate
                own = jnp.concatenate([own] * 4, axis=1)
                at = (s, slice(None), pl.ds(start, 128))
                rows[at] = rows[at] + jnp.where(group == x0 * 2 + c, own, 0.0)
                for n in range(blocks):
                    lead.append(rows[s, :, n * block : (n + 1) * block].astype(bf16))
            dealt = dot(jnp.concatenate(lead, axis=0), deal).astype(bf16)
            for k in range(4):
                for n in range(blocks):
                    part = dealt[(k * blocks + n) * height : (k * blocks + n + 1) * height]
                    cols = slice(n * 128, (n + 1) * 128)
                    for h in range(block // 256):
                        to = (g * 4 + k) * (block // 256) + h
                        near[to, :, cols] = part[:, h * 128 : (h + 1) * 128]
                        far[to, :, cols] = part[:, block // 2 + h * 128 : block // 2 + (h + 1) * 128]
            return 0

        lax.fori_loop(0, slots // 4, four, 0)

    pl.when(found <= 16)(lambda: spread(16, 512, mine, theirs))
    pl.when(found > 16)(lambda: spread(slots, 256, mine_wide, theirs_wide))


def pack(layer_live, grad_parts, momentum):
    _, _, rows, cols = grad_parts.shape
    half = jax.ShapeDtypeStruct((32, rows, cols // 4), bf16)
    wide = jax.ShapeDtypeStruct((32, rows, cols // 2), bf16)
    grad_parts = pltpu.with_memory_space_constraint(grad_parts, pltpu.HBM)
    momentum = pltpu.with_memory_space_constraint(momentum, pltpu.HBM)
    return pl.pallas_call(
        pack_body,
        in_specs=[whole(pltpu.SMEM), whole(pl.ANY), whole(pl.ANY)],
        out_specs=[whole()] * 4 + [whole(pltpu.SMEM)],
        out_shape=[half, half, wide, wide, jax.ShapeDtypeStruct((1,), i32)],
        scratch_shapes=[
            pltpu.VMEM((32, rows, cols), f32),
            pltpu.VMEM(momentum.shape, f32),
            pltpu.SMEM((32,), i32),
            pltpu.SemaphoreType.DMA((32,)),
            pltpu.SemaphoreType.DMA,
        ],
        compiler_params=room(16),
        name="pack",
    )(layer_live, grad_parts, momentum)


def total_body(parts, out):
    total = jnp.sum(parts[...].astype(f32), axis=0).astype(bf16)
    for z in range(out.shape[0]):
        out[z] = total


def total(parts, copies):
    return pl.pallas_call(
        total_body,
        in_specs=[whole()],
        out_specs=whole(),
        out_shape=jax.ShapeDtypeStruct((copies,) + parts.shape[1:], bf16),
        compiler_params=room(4),
        name="total",
    )(parts)


def gram_body(source, out):
    s = source[...].reshape(source.shape[0] * source.shape[1], -1)
    g = lax.dot_general(s, s, (((1,), (1,)), ((), ())), preferred_element_type=f32)
    out[:64] = g[:64]
    out[64:, 64:] = g[64:128, 64:]
    out[64:, :64] = g[128:, 128:]


def gram(source):
    return pl.pallas_call(
        gram_body,
        in_specs=[whole()],
        out_specs=whole(),
        out_shape=jax.ShapeDtypeStruct((128, 192), f32),
        compiler_params=room(4),
        name="gram",
    )(source)


def unfolded(g):
    top, low = g[:64], g[64:]
    middle = jnp.concatenate([top[:, 64:128].T, low[:, 64:]], axis=1)
    bottom = jnp.concatenate([top[:, 128:].T, low[:, 128:].T, low[:, :64]], axis=1)
    return jnp.concatenate([top, middle, bottom], axis=0)


def schulz_body(gram_a, gram_b, source, out):
    g = unfolded(gram_a[...] + gram_b[...])
    rows = g.shape[0]
    own_rows = source.shape[1]
    z = lax.axis_index("dp")
    row = lax.broadcasted_iota(i32, g.shape, 0)
    col = lax.broadcasted_iota(i32, g.shape, 1)
    eye = row == col
    square = jnp.sum(jnp.sum(jnp.where(eye, g, 0.0), axis=1, keepdims=True), axis=0, keepdims=True)
    scale = 1.0 / (jnp.sqrt(square) + norm_eps)
    g = g * scale * scale
    pick = (
        lax.broadcasted_iota(i32, (own_rows, rows), 1)
        == lax.broadcasted_iota(i32, (own_rows, rows), 0) + z * own_rows
    )
    gh = halves(g)
    for iteration in range(ITERS - 1):
        w = second_coef * g + third_coef * dot3(gh, gh) + jnp.where(eye, first_coef, 0.0)
        wh = halves(w)
        lead = dot3(halves(lead), wh) if iteration else dot(pick.astype(bf16), wh[0]) + dot(pick.astype(bf16), wh[1])
        g = dot3(halves(dot3(wh, gh)), wh)
        gh = halves(g)
    once = dot3(halves(lead), gh)
    twice = dot3(halves(once), gh)
    lead = first_coef * lead + second_coef * once + third_coef * twice
    lead = halves(lead * (scale * math.sqrt(2048.0)))
    s = source[...].reshape(rows, -1)
    result = dot(lead[0], s) + dot(lead[1], s)
    own = source[z].astype(f32)
    lane = lax.broadcasted_iota(i32, (own_rows, 128), 1)
    for j in range(out.shape[0]):
        yy, t = j // 4, j % 4
        up = result[:, yy * 128 : (yy + 1) * 128]
        low = own[:, yy * 128 : (yy + 1) * 128]
        up = pltpu.roll(up, 128 - 32 * t, 1) if t else up
        low = pltpu.roll(low, (160 - 32 * t) % 128, 1) if t != 1 else low
        out[j] = jnp.where(lane < 32, up, low).astype(bf16)


def schulz(gram_a, gram_b, source):
    return pl.pallas_call(
        schulz_body,
        in_specs=[whole(), whole(), whole()],
        out_specs=whole(),
        out_shape=jax.ShapeDtypeStruct((source.shape[2] // 32, source.shape[1], 128), bf16),
        compiler_params=room(8),
        name="schulz",
    )(gram_a, gram_b, source)


def place_body(live, came, mom_in, mom, orth):
    found = 0
    for m in range(mom.shape[0]):
        here = live[m] > 0
        got = came[jnp.minimum(found, came.shape[0] - 1)].astype(f32)
        found = found + jnp.where(here, 1, 0)
        mom[m] = jnp.where(here, pltpu.roll(got, 96, 1)[:, :32], mom_in[m])
        orth[m] = jnp.where(here, got[:, :32], 0.0).astype(bf16)


def place(layer_live, came, momentum):
    return pl.pallas_call(
        place_body,
        in_specs=[whole(pltpu.SMEM), whole(), whole()],
        out_specs=[whole(), whole()],
        out_shape=[jax.ShapeDtypeStruct(momentum.shape, f32), jax.ShapeDtypeStruct(momentum.shape, bf16)],
        compiler_params=room(4),
        name="place",
    )(layer_live, came, momentum)


def swapped(x, axis):
    return lax.ppermute(x, axis, [(0, 1), (1, 0)])


def finish(mine, came, wide, layer_live, momentum):
    chip_sum = (mine.astype(f32) + came.astype(f32)).astype(bf16)
    parts = lax.all_to_all(chip_sum, CHIPS, 0, 0, tiled=True)
    copies = total(parts, lax.axis_size("dp"))
    source = lax.all_to_all(copies, "dp", 0, 0, tiled=True)
    partial = gram(source)
    if wide:
        update = schulz(partial, swapped(partial, "c"), source)
        back = lax.all_to_all(update, CHIPS, 0, 0, tiled=True)
    else:
        partial = partial + swapped(partial, "c")
        update = schulz(partial, swapped(partial, "x0"), source)
        back = lax.all_to_all(update, OWNERS, 0, 0, tiled=True)
    return tuple(place(layer_live, back, momentum))


def per_device(grad_parts, momentum, layer_live):
    mine, theirs, mine_wide, theirs_wide, count = pack(layer_live, grad_parts, momentum)
    came = swapped(theirs, "c")

    def narrow(mine, came, mine_wide, theirs_wide, *rest):
        return finish(mine, came, False, *rest)

    def wide(mine, came, mine_wide, theirs_wide, *rest):
        return finish(mine_wide, swapped(theirs_wide, "c"), True, *rest)

    return lax.cond(count[0] > 16, wide, narrow, mine, came, mine_wide, theirs_wide, layer_live, momentum)


def solution(mesh):
    torus = Mesh(
        mesh.devices.reshape(mesh.shape["dp"], mesh.shape["rep"], 2, 2, 2),
        ("dp", "rep", "x1", "x0", "c"),
    )
    return jax.shard_map(
        per_device,
        mesh=torus,
        in_specs=(P(COLS, None, "dp", None), P(None, "dp", COLS), P()),
        out_specs=(P(None, "dp", COLS), P(None, "dp", COLS)),
        check_vma=False,
    )
```

```python
import functools
import math

import jax
import jax.numpy as jnp
from jax import lax
from jax.experimental import pallas as pl
from jax.experimental.pallas import tpu as pltpu
from jax.sharding import Mesh
from jax.sharding import PartitionSpec as P

ITERS = 5
COLS = ("rep", "x1", "x0", "c")
CHIPS = ("rep", "x1", "x0")
OWNERS = ("rep", "x1")

decay_rate = 0.95
first_coef = 3.4445
second_coef = -4.775
third_coef = 2.0315
norm_eps = 1e-07

bf16 = jnp.bfloat16
f32 = jnp.float32
i32 = jnp.int32


def whole(space=pltpu.VMEM):
    return pl.BlockSpec(memory_space=space)


def room(mib):
    return pltpu.CompilerParams(vmem_limit_bytes=mib << 20)


def halves(a):
    high = a.astype(bf16)
    return high, (a - high.astype(f32)).astype(bf16)


def dot(a, b):
    return jnp.dot(a, b, preferred_element_type=f32)


def dot3(lefts, b):
    rows = [high.shape[0] for high, _ in lefts]
    highs = jnp.concatenate([high for high, _ in lefts], axis=0)
    both = dot(jnp.concatenate([highs] + [low for _, low in lefts], axis=0), b[0])
    side = dot(highs, b[1])
    outs, at, total = [], 0, sum(rows)
    for r in rows:
        outs.append(both[at : at + r] + (side[at : at + r] + both[total + at : total + at + r]))
        at += r
    return outs


def pack_body(live, grads, mom, mine, theirs, mine_wide, theirs_wide, count, rows, own_mom, holder, row_sems, mom_sem):
    slots, height, width = rows.shape
    mats = live.shape[0]
    fetch_mom = pltpu.make_async_copy(mom, own_mom, mom_sem)
    fetch_mom.start()
    for s in range(slots):
        holder[s] = 0
    found = 0
    for m in range(mats):
        holder[found] = m
        found = found + jnp.where(live[m] > 0, 1, 0)
    count[0] = found
    used = jnp.where(found > 16, slots, 16)

    def fetch(s):
        return pltpu.make_async_copy(grads.at[0, holder[s]], rows.at[s], row_sems.at[s])

    def begin(s, _):
        fetch(s).start()
        return 0

    lax.fori_loop(0, used, begin, 0)
    rep, x1 = lax.axis_index("rep"), lax.axis_index("x1")
    x0, c = lax.axis_index("x0"), lax.axis_index("c")
    group = lax.broadcasted_iota(i32, (height, 128), 1) // 32
    start = pl.multiple_of((rep * 2 + x1) * 128, 128)
    fetch_mom.wait()

    def spread(slots, block, near, far):
        blocks = width // block
        old = lax.broadcasted_iota(i32, (block, block), 0)
        new = lax.broadcasted_iota(i32, (block, block), 1)
        far_half = ((old // 32 % 2) ^ c) * (block // 2)
        if block == 512:
            target = far_half + (old // 64 % 2) * 128 + old // 128 * 32 + old % 32
        else:
            target = far_half + old // 128 * 64 + (old // 64 % 2) * 32 + old % 32
        deal = jnp.where(target == new, 1.0, 0.0).astype(bf16)

        def eight(g, _):
            lead = []
            for k in range(8):
                s = g * 8 + k
                fetch(s).wait()
                own = own_mom[holder[s]] * decay_rate
                own = jnp.concatenate([own] * 4, axis=1)
                at = (s, slice(None), pl.ds(start, 128))
                rows[at] = rows[at] + jnp.where(group == x0 * 2 + c, own, 0.0)
                for n in range(blocks):
                    lead.append(rows[s, :, n * block : (n + 1) * block].astype(bf16))
            dealt = dot(jnp.concatenate(lead, axis=0), deal).astype(bf16)
            for k in range(8):
                for n in range(blocks):
                    part = dealt[(k * blocks + n) * height : (k * blocks + n + 1) * height]
                    cols = slice(n * 128, (n + 1) * 128)
                    for h in range(block // 256):
                        to = (g * 8 + k) * (block // 256) + h
                        near[to, :, cols] = part[:, h * 128 : (h + 1) * 128]
                        far[to, :, cols] = part[:, block // 2 + h * 128 : block // 2 + (h + 1) * 128]
            return 0

        lax.fori_loop(0, slots // 8, eight, 0)

    pl.when(found <= 16)(lambda: spread(16, 512, mine, theirs))
    pl.when(found > 16)(lambda: spread(slots, 256, mine_wide, theirs_wide))


def pack(layer_live, grad_parts, momentum):
    _, _, rows, cols = grad_parts.shape
    half = jax.ShapeDtypeStruct((32, rows, cols // 4), bf16)
    wide = jax.ShapeDtypeStruct((32, rows, cols // 2), bf16)
    grad_parts = pltpu.with_memory_space_constraint(grad_parts, pltpu.HBM)
    momentum = pltpu.with_memory_space_constraint(momentum, pltpu.HBM)
    return pl.pallas_call(
        pack_body,
        in_specs=[whole(pltpu.SMEM), whole(pl.ANY), whole(pl.ANY)],
        out_specs=[whole()] * 4 + [whole(pltpu.SMEM)],
        out_shape=[half, half, wide, wide, jax.ShapeDtypeStruct((1,), i32)],
        scratch_shapes=[
            pltpu.VMEM((32, rows, cols), f32),
            pltpu.VMEM(momentum.shape, f32),
            pltpu.SMEM((32,), i32),
            pltpu.SemaphoreType.DMA((32,)),
            pltpu.SemaphoreType.DMA,
        ],
        compiler_params=room(16),
        name="pack",
    )(layer_live, grad_parts, momentum)


def total_body(parts, out):
    total = jnp.sum(parts[...].astype(f32), axis=0).astype(bf16)
    for z in range(out.shape[0]):
        out[z] = total


def total(parts, copies):
    return pl.pallas_call(
        total_body,
        in_specs=[whole()],
        out_specs=whole(),
        out_shape=jax.ShapeDtypeStruct((copies,) + parts.shape[1:], bf16),
        compiler_params=room(4),
        name="total",
    )(parts)


def gram_body(source, out):
    s = source[...].reshape(source.shape[0] * source.shape[1], -1)
    g = lax.dot_general(s, s, (((1,), (1,)), ((), ())), preferred_element_type=f32)
    out[:64] = g[:64]
    out[64:, 64:] = g[64:128, 64:]
    out[64:, :64] = g[128:, 128:]


def gram(source):
    return pl.pallas_call(
        gram_body,
        in_specs=[whole()],
        out_specs=whole(),
        out_shape=jax.ShapeDtypeStruct((128, 192), f32),
        compiler_params=room(4),
        name="gram",
    )(source)


def unfolded(g):
    top, low = g[:64], g[64:]
    middle = jnp.concatenate([top[:, 64:128].T, low[:, 64:]], axis=1)
    bottom = jnp.concatenate([top[:, 128:].T, low[:, 128:].T, low[:, :64]], axis=1)
    return jnp.concatenate([top, middle, bottom], axis=0)


def schulz_body(gram_a, gram_b, source, out):
    g = unfolded(gram_a[...] + gram_b[...])
    rows = g.shape[0]
    own_rows = source.shape[1]
    z = lax.axis_index("dp")
    row = lax.broadcasted_iota(i32, g.shape, 0)
    col = lax.broadcasted_iota(i32, g.shape, 1)
    eye = row == col
    square = jnp.sum(jnp.sum(jnp.where(eye, g, 0.0), axis=1, keepdims=True), axis=0, keepdims=True)
    scale = 1.0 / (jnp.sqrt(square) + norm_eps)
    g = g * scale * scale
    pick = (
        lax.broadcasted_iota(i32, (own_rows, rows), 1)
        == lax.broadcasted_iota(i32, (own_rows, rows), 0) + z * own_rows
    )
    gh = halves(g)
    lead = pick.astype(f32)
    for iteration in range(ITERS - 1):
        w = second_coef * g + third_coef * dot3([gh], gh)[0] + jnp.where(eye, first_coef, 0.0)
        wh = halves(w)
        turned = halves(dot3([wh], gh)[0])
        g, lead = dot3([turned, halves(lead)], wh)
        gh = halves(g)
    once = dot3([halves(lead)], gh)[0]
    twice = dot3([halves(once)], gh)[0]
    lead = first_coef * lead + second_coef * once + third_coef * twice
    lead = halves(lead * (scale * math.sqrt(2048.0)))
    s = source[...].reshape(rows, -1)
    result = dot(lead[0], s) + dot(lead[1], s)
    own = source[z].astype(f32)
    half = own_rows // 2
    group = lax.broadcasted_iota(i32, (half, 128), 1) // 32
    for j in range(out.shape[0]):
        yy, t = j // 4, j % 4
        piece = None
        for place_at, (whole_rows, first) in enumerate(((result, 0), (result, half), (own, 0), (own, half))):
            part = whole_rows[first : first + half, yy * 128 : (yy + 1) * 128]
            turn = (place_at - t) * 32 % 128
            part = pltpu.roll(part, turn, 1) if turn else part
            piece = part if piece is None else jnp.where(group == place_at, part, piece)
        out[j] = piece.astype(bf16)


def schulz(gram_a, gram_b, source):
    return pl.pallas_call(
        schulz_body,
        in_specs=[whole(), whole(), whole()],
        out_specs=whole(),
        out_shape=jax.ShapeDtypeStruct((source.shape[2] // 32, source.shape[1] // 2, 128), bf16),
        compiler_params=room(8),
        name="schulz",
    )(gram_a, gram_b, source)


def place_body(live, came, mom_in, mom, orth):
    found = 0
    for m in range(mom.shape[0]):
        here = live[m] > 0
        got = came[jnp.minimum(found, came.shape[0] - 1)].astype(f32)
        found = found + jnp.where(here, 1, 0)
        parts = [got[:, :32]] + [pltpu.roll(got, 128 - 32 * t, 1)[:, :32] for t in range(1, 4)]
        mom[m] = jnp.where(here, jnp.concatenate(parts[2:], axis=0), mom_in[m])
        orth[m] = jnp.where(here, jnp.concatenate(parts[:2], axis=0), 0.0).astype(bf16)


def place(layer_live, came, momentum):
    return pl.pallas_call(
        place_body,
        in_specs=[whole(pltpu.SMEM), whole(), whole()],
        out_specs=[whole(), whole()],
        out_shape=[jax.ShapeDtypeStruct(momentum.shape, f32), jax.ShapeDtypeStruct(momentum.shape, bf16)],
        compiler_params=room(4),
        name="place",
    )(layer_live, came, momentum)


def swapped(x, axis):
    return lax.ppermute(x, axis, [(0, 1), (1, 0)])


def finish(mine, came, wide, layer_live, momentum):
    chip_sum = (mine.astype(f32) + came.astype(f32)).astype(bf16)
    parts = lax.all_to_all(chip_sum, CHIPS, 0, 0, tiled=True)
    copies = total(parts, lax.axis_size("dp"))
    source = lax.all_to_all(copies, "dp", 0, 0, tiled=True)
    partial = gram(source)
    if wide:
        update = schulz(partial, swapped(partial, "c"), source)
        back = lax.all_to_all(update, CHIPS, 0, 0, tiled=True)
    else:
        partial = partial + swapped(partial, "c")
        update = schulz(partial, swapped(partial, "x0"), source)
        back = lax.all_to_all(update, OWNERS, 0, 0, tiled=True)
    return tuple(place(layer_live, back, momentum))


def per_device(grad_parts, momentum, layer_live):
    mine, theirs, mine_wide, theirs_wide, count = pack(layer_live, grad_parts, momentum)
    came = swapped(theirs, "c")

    def narrow(mine, came, mine_wide, theirs_wide, *rest):
        return finish(mine, came, False, *rest)

    def wide(mine, came, mine_wide, theirs_wide, *rest):
        return finish(mine_wide, swapped(theirs_wide, "c"), True, *rest)

    return lax.cond(count[0] > 16, wide, narrow, mine, came, mine_wide, theirs_wide, layer_live, momentum)


def solution(mesh):
    torus = Mesh(
        mesh.devices.reshape(mesh.shape["dp"], mesh.shape["rep"], 2, 2, 2),
        ("dp", "rep", "x1", "x0", "c"),
    )
    return jax.shard_map(
        per_device,
        mesh=torus,
        in_specs=(P(COLS, None, "dp", None), P(None, "dp", COLS), P()),
        out_specs=(P(None, "dp", COLS), P(None, "dp", COLS)),
        check_vma=False,
    )
```

```python
import functools
import math

import jax
import jax.numpy as jnp
from jax import lax
from jax.experimental import pallas as pl
from jax.experimental.pallas import tpu as pltpu
from jax.sharding import Mesh
from jax.sharding import PartitionSpec as P

ITERS = 5
COLS = ("rep", "x1", "x0", "c")
CHIPS = ("rep", "x1", "x0")
OWNERS = ("rep", "x1")

decay_rate = 0.95
first_coef = 3.4445
second_coef = -4.775
third_coef = 2.0315
norm_eps = 1e-07

bf16 = jnp.bfloat16
f32 = jnp.float32
i32 = jnp.int32


def whole(space=pltpu.VMEM):
    return pl.BlockSpec(memory_space=space)


def room(mib):
    return pltpu.CompilerParams(vmem_limit_bytes=mib << 20)


def halves(a):
    high = a.astype(bf16)
    return high, (a - high.astype(f32)).astype(bf16)


def dot(a, b):
    return jnp.dot(a, b, preferred_element_type=f32)


def dot3(lefts, b):
    rows = [high.shape[0] for high, _ in lefts]
    highs = jnp.concatenate([high for high, _ in lefts], axis=0)
    both = dot(jnp.concatenate([highs] + [low for _, low in lefts], axis=0), b[0])
    side = dot(highs, b[1])
    outs, at, total = [], 0, sum(rows)
    for r in rows:
        outs.append(both[at : at + r] + (side[at : at + r] + both[total + at : total + at + r]))
        at += r
    return outs


def pack_body(live, grads, mom, mine, theirs, mine_wide, theirs_wide, count, rows, own_mom, holder, row_sems, mom_sem):
    slots, height, width = rows.shape
    mats = live.shape[0]
    fetch_mom = pltpu.make_async_copy(mom, own_mom, mom_sem)
    fetch_mom.start()
    for s in range(slots):
        holder[s] = 0
    found = 0
    for m in range(mats):
        holder[found] = m
        found = found + jnp.where(live[m] > 0, 1, 0)
    count[0] = found
    used = jnp.where(found > 16, slots, 16)

    def fetch(s):
        return pltpu.make_async_copy(grads.at[0, holder[s]], rows.at[s], row_sems.at[s])

    def begin(s, _):
        fetch(s).start()
        return 0

    lax.fori_loop(0, used, begin, 0)
    rep, x1 = lax.axis_index("rep"), lax.axis_index("x1")
    x0, c = lax.axis_index("x0"), lax.axis_index("c")
    group = lax.broadcasted_iota(i32, (height, 128), 1) // 32
    start = pl.multiple_of((rep * 2 + x1) * 128, 128)
    fetch_mom.wait()

    def spread(slots, block, near, far):
        blocks = width // block
        old = lax.broadcasted_iota(i32, (block, block), 0)
        new = lax.broadcasted_iota(i32, (block, block), 1)
        far_half = ((old // 32 % 2) ^ c) * (block // 2)
        if block == 512:
            target = far_half + (old // 64 % 2) * 128 + old // 128 * 32 + old % 32
        else:
            target = far_half + old // 128 * 64 + (old // 64 % 2) * 32 + old % 32
        deal = jnp.where(target == new, 1.0, 0.0).astype(bf16)

        def sixteen(g, _):
            lead = []
            for k in range(16):
                s = g * 16 + k
                fetch(s).wait()
                own = own_mom[holder[s]] * decay_rate
                own = jnp.concatenate([own] * 4, axis=1)
                at = (s, slice(None), pl.ds(start, 128))
                rows[at] = rows[at] + jnp.where(group == x0 * 2 + c, own, 0.0)
                for n in range(blocks):
                    lead.append(rows[s, :, n * block : (n + 1) * block].astype(bf16))
            dealt = dot(jnp.concatenate(lead, axis=0), deal).astype(bf16)
            for k in range(16):
                for n in range(blocks):
                    part = dealt[(k * blocks + n) * height : (k * blocks + n + 1) * height]
                    cols = slice(n * 128, (n + 1) * 128)
                    for h in range(block // 256):
                        to = (g * 16 + k) * (block // 256) + h
                        near[to, :, cols] = part[:, h * 128 : (h + 1) * 128]
                        far[to, :, cols] = part[:, block // 2 + h * 128 : block // 2 + (h + 1) * 128]
            return 0

        lax.fori_loop(0, slots // 16, sixteen, 0)

    pl.when(found <= 16)(lambda: spread(16, 512, mine, theirs))
    pl.when(found > 16)(lambda: spread(slots, 256, mine_wide, theirs_wide))


def pack(layer_live, grad_parts, momentum):
    _, _, rows, cols = grad_parts.shape
    half = jax.ShapeDtypeStruct((32, rows, cols // 4), bf16)
    wide = jax.ShapeDtypeStruct((32, rows, cols // 2), bf16)
    grad_parts = pltpu.with_memory_space_constraint(grad_parts, pltpu.HBM)
    momentum = pltpu.with_memory_space_constraint(momentum, pltpu.HBM)
    return pl.pallas_call(
        pack_body,
        in_specs=[whole(pltpu.SMEM), whole(pl.ANY), whole(pl.ANY)],
        out_specs=[whole()] * 4 + [whole(pltpu.SMEM)],
        out_shape=[half, half, wide, wide, jax.ShapeDtypeStruct((1,), i32)],
        scratch_shapes=[
            pltpu.VMEM((32, rows, cols), f32),
            pltpu.VMEM(momentum.shape, f32),
            pltpu.SMEM((32,), i32),
            pltpu.SemaphoreType.DMA((32,)),
            pltpu.SemaphoreType.DMA,
        ],
        compiler_params=room(16),
        name="pack",
    )(layer_live, grad_parts, momentum)


def total_body(parts, out):
    total = jnp.sum(parts[...].astype(f32), axis=0).astype(bf16)
    for z in range(out.shape[0]):
        out[z] = total


def total(parts, copies):
    return pl.pallas_call(
        total_body,
        in_specs=[whole()],
        out_specs=whole(),
        out_shape=jax.ShapeDtypeStruct((copies,) + parts.shape[1:], bf16),
        compiler_params=room(4),
        name="total",
    )(parts)


def gram_body(source, out):
    s = source[...].reshape(source.shape[0] * source.shape[1], -1)
    g = lax.dot_general(s, s, (((1,), (1,)), ((), ())), preferred_element_type=f32)
    out[:64] = g[:64]
    out[64:, 64:] = g[64:128, 64:]
    out[64:, :64] = g[128:, 128:]


def gram(source):
    return pl.pallas_call(
        gram_body,
        in_specs=[whole()],
        out_specs=whole(),
        out_shape=jax.ShapeDtypeStruct((128, 192), f32),
        compiler_params=room(4),
        name="gram",
    )(source)


def unfolded(g):
    top, low = g[:64], g[64:]
    middle = jnp.concatenate([top[:, 64:128].T, low[:, 64:]], axis=1)
    bottom = jnp.concatenate([top[:, 128:].T, low[:, 128:].T, low[:, :64]], axis=1)
    return jnp.concatenate([top, middle, bottom], axis=0)


def schulz_body(gram_a, gram_b, source, out):
    g = unfolded(gram_a[...] + gram_b[...])
    rows = g.shape[0]
    own_rows = source.shape[1]
    z = lax.axis_index("dp")
    row = lax.broadcasted_iota(i32, g.shape, 0)
    col = lax.broadcasted_iota(i32, g.shape, 1)
    eye = row == col
    square = jnp.sum(jnp.sum(jnp.where(eye, g, 0.0), axis=1, keepdims=True), axis=0, keepdims=True)
    scale = 1.0 / (jnp.sqrt(square) + norm_eps)
    g = g * scale * scale
    pick = (
        lax.broadcasted_iota(i32, (own_rows, rows), 1)
        == lax.broadcasted_iota(i32, (own_rows, rows), 0) + z * own_rows
    )
    gh = halves(g)
    lead = pick.astype(f32)
    for iteration in range(ITERS - 1):
        w = second_coef * g + third_coef * dot3([gh], gh)[0] + jnp.where(eye, first_coef, 0.0)
        wh = halves(w)
        turned = halves(dot3([wh], gh)[0])
        g, lead = dot3([turned, halves(lead)], wh)
        gh = halves(g)
    once = dot3([halves(lead)], gh)[0]
    twice = dot3([halves(once)], gh)[0]
    lead = first_coef * lead + second_coef * once + third_coef * twice
    lead = halves(lead * (scale * math.sqrt(2048.0)))
    s = source[...].reshape(rows, -1)
    result = dot(lead[0], s) + dot(lead[1], s)
    own = source[z].astype(f32)
    half = own_rows // 2
    group = lax.broadcasted_iota(i32, (half, 128), 1) // 32
    for j in range(out.shape[0]):
        yy, t = j // 4, j % 4
        piece = None
        for place_at, (whole_rows, first) in enumerate(((result, 0), (result, half), (own, 0), (own, half))):
            part = whole_rows[first : first + half, yy * 128 : (yy + 1) * 128]
            turn = (place_at - t) * 32 % 128
            part = pltpu.roll(part, turn, 1) if turn else part
            piece = part if piece is None else jnp.where(group == place_at, part, piece)
        out[j] = piece.astype(bf16)


def schulz(gram_a, gram_b, source):
    return pl.pallas_call(
        schulz_body,
        in_specs=[whole(), whole(), whole()],
        out_specs=whole(),
        out_shape=jax.ShapeDtypeStruct((source.shape[2] // 32, source.shape[1] // 2, 128), bf16),
        compiler_params=room(8),
        name="schulz",
    )(gram_a, gram_b, source)


def place_body(live, came, mom_in, mom, orth):
    found = 0
    for m in range(mom.shape[0]):
        here = live[m] > 0
        got = came[jnp.minimum(found, came.shape[0] - 1)].astype(f32)
        found = found + jnp.where(here, 1, 0)
        parts = [got[:, :32]] + [pltpu.roll(got, 128 - 32 * t, 1)[:, :32] for t in range(1, 4)]
        mom[m] = jnp.where(here, jnp.concatenate(parts[2:], axis=0), mom_in[m])
        orth[m] = jnp.where(here, jnp.concatenate(parts[:2], axis=0), 0.0).astype(bf16)


def place(layer_live, came, momentum):
    return pl.pallas_call(
        place_body,
        in_specs=[whole(pltpu.SMEM), whole(), whole()],
        out_specs=[whole(), whole()],
        out_shape=[jax.ShapeDtypeStruct(momentum.shape, f32), jax.ShapeDtypeStruct(momentum.shape, bf16)],
        compiler_params=room(4),
        name="place",
    )(layer_live, came, momentum)


def swapped(x, axis):
    return lax.ppermute(x, axis, [(0, 1), (1, 0)])


def finish(mine, came, wide, layer_live, momentum):
    chip_sum = (mine.astype(f32) + came.astype(f32)).astype(bf16)
    parts = lax.all_to_all(chip_sum, CHIPS, 0, 0, tiled=True)
    copies = total(parts, lax.axis_size("dp"))
    source = lax.all_to_all(copies, "dp", 0, 0, tiled=True)
    partial = gram(source)
    if wide:
        update = schulz(partial, swapped(partial, "c"), source)
        back = lax.all_to_all(update, CHIPS, 0, 0, tiled=True)
    else:
        partial = partial + swapped(partial, "c")
        update = schulz(partial, swapped(partial, "x0"), source)
        back = lax.all_to_all(update, OWNERS, 0, 0, tiled=True)
    return tuple(place(layer_live, back, momentum))


def per_device(grad_parts, momentum, layer_live):
    mine, theirs, mine_wide, theirs_wide, count = pack(layer_live, grad_parts, momentum)
    came = swapped(theirs, "c")

    def narrow(mine, came, mine_wide, theirs_wide, *rest):
        return finish(mine, came, False, *rest)

    def wide(mine, came, mine_wide, theirs_wide, *rest):
        return finish(mine_wide, swapped(theirs_wide, "c"), True, *rest)

    return lax.cond(count[0] > 16, wide, narrow, mine, came, mine_wide, theirs_wide, layer_live, momentum)


def solution(mesh):
    torus = Mesh(
        mesh.devices.reshape(mesh.shape["dp"], mesh.shape["rep"], 2, 2, 2),
        ("dp", "rep", "x1", "x0", "c"),
    )
    return jax.shard_map(
        per_device,
        mesh=torus,
        in_specs=(P(COLS, None, "dp", None), P(None, "dp", COLS), P()),
        out_specs=(P(None, "dp", COLS), P(None, "dp", COLS)),
        check_vma=False,
    )
```
